32 devices in a mesh: gx: 2 (over core), gy: 4 (over y, x), rep: 4 (over z).
Axes of the slice: x: 2, y: 2, z: 4, core: 2. Of those that a mesh axis runs over, the one named last changes fastest.
Arguments:
- generator: float32 [384, 384], P('gx', 'gy'), may hold values from -1.25 to 1.25
Outputs:
- propagator: float32 [384, 384], P('gx', 'gy')
The draws below stay inside these ranges and needn't reach their ends.
All inputs are finite; a program needn't handle non-finite values.
Results may differ from the reference program's by a relative error of at most 0.0003.
Values sent between devices are 32-bit elements.
A program may use at most 64 MiB of HBM per device.

```python
import jax
import jax.numpy as jnp
from jax import lax

DEGREE = 8
SQUARINGS = 4
ORDER = 384


def level_of(rng, dims, split, least, largest):
    factor_of = 1.0
    for axis_at, parts in split:
        steps = jax.random.uniform(jax.random.fold_in(jax.random.fold_in(rng, 6), axis_at), (parts,), jnp.float32, least / len(split), largest / len(split))
        factor_of = factor_of * jnp.repeat(jnp.exp(steps), dims[axis_at] // parts).reshape((-1,) + (1,) * (len(dims) - 1 - axis_at))
    return factor_of


def scatter_about(own_key, extent, width, most, pieces=(), kind=jnp.bfloat16):
    array = jax.random.normal(own_key, extent, jnp.float32) * width
    if len(pieces) > 0:
        array = level_of(own_key, extent, pieces, -0.22, 0.18) * array
    return jnp.clip(array, min=-most, max=most).astype(kind)


def setup_inputs(seed: int = 0) -> dict:
    key_of = jax.random.split(jax.random.key(seed), 2)
    return {
        "generator": scatter_about(key_of[0], (ORDER, ORDER), (ORDER // 16) ** -0.5, 1.25, ((0, 2), (1, 4)), jnp.float32),
    }


def multiply(first, second):
    return jnp.dot(first, second, precision=lax.Precision.HIGHEST, preferred_element_type=jnp.float32)


def reference(generator):
    scaled = generator / (2.0 ** SQUARINGS)
    unit_matrix = jnp.eye(ORDER, dtype=jnp.float32)
    taylor = unit_matrix + scaled / DEGREE
    for power in range(DEGREE - 1, 0, -1):
        taylor = unit_matrix + multiply(scaled, taylor) / power
    for square_index in range(SQUARINGS):
        taylor = multiply(taylor, taylor)
    return taylor
```

```python
import functools
import math

import jax
import jax.numpy as jnp
from jax import lax
from jax.experimental import pallas as pl
from jax.experimental.pallas import tpu as pltpu
from jax.sharding import PartitionSpec as P

DEGREE = 8
SQUARINGS = 4
CHUNKS = 2
VMEM_BUDGET = 40 * 2**20

ROOT = math.sqrt(177.0)
X3 = 2.0 / 3.0
X1 = X3 * (1.0 + ROOT) / 88.0
X2 = X3 * (1.0 + ROOT) / 352.0
X4 = (-271.0 + 29.0 * ROOT) / (315.0 * X3)
X5 = 11.0 * (-1.0 + ROOT) / (1260.0 * X3)
X6 = 11.0 * (-9.0 + ROOT) / (5040.0 * X3)
X7 = (89.0 - ROOT) / (5040.0 * X3 * X3)
Y2 = (857.0 - 58.0 * ROOT) / 630.0


def split(x):
    high = x.astype(jnp.bfloat16)
    return high, (x - high.astype(jnp.float32)).astype(jnp.bfloat16)


def times(x, y):
    dot = functools.partial(jnp.dot, preferred_element_type=jnp.float32)
    return dot(x[0], y[0]) + (dot(x[0], y[1]) + dot(x[1], y[0]))


def flipped(index, mask):
    bit = 1
    while bit <= mask:
        if mask & bit:
            index = index + (1 - 2 * ((index // bit) % 2)) * bit
        bit *= 2
    return index


def whole_kernel(nx, ny, gen, out, parts, th, tl, send, land, relay, relayed, own):
    rows, cols = out.shape
    order = ny * cols
    span = rows // CHUNKS
    gx, gy = lax.axis_index("gx"), lax.axis_index("gy")

    barrier = pltpu.get_barrier_semaphore()
    for mask in range(1, ny):
        pl.semaphore_signal(barrier, inc=1, device_id={"gy": flipped(gy, mask)})
    for dx in range(1, nx):
        pl.semaphore_signal(barrier, inc=1, device_id={"gx": (gx + dx) % nx})
    mine = pltpu.make_async_copy(gen, parts.at[gx, 0], own)
    mine.start()
    pl.semaphore_wait(barrier, ny + nx - 2)

    out_copies, in_copies, passed = [], [], []

    def pass_on(mask, c, src):
        piece = pl.ds(c * span, span)
        for dx in range(1, nx):
            copy = pltpu.make_async_remote_copy(
                src, parts.at[gx, mask, piece, :],
                relay.at[dx - 1, mask, c], relayed.at[dx - 1, mask, c],
                device_id={"gx": (gx + dx) % nx},
            )
            copy.start()
            passed.append(copy)

    for c in range(CHUNKS):
        piece = pl.ds(c * span, span)
        for mask in range(ny - 1, 0, -1):
            copy = pltpu.make_async_remote_copy(
                gen.at[piece, :], parts.at[gx, mask, piece, :],
                send.at[mask, c], land.at[mask, c],
                device_id={"gy": flipped(gy, mask)},
            )
            copy.start()
            out_copies.append(copy)
    for c in range(CHUNKS):
        pass_on(0, c, gen.at[pl.ds(c * span, span), :])
    for c in range(CHUNKS):
        for mask in range(1, ny):
            piece = pl.ds(c * span, span)
            out_copies[c * (ny - 1) + ny - 1 - mask].wait_recv()
            pass_on(mask, c, parts.at[gx, mask, piece, :])
    mine.wait()
    for copy in passed:
        copy.wait_recv()

    per = rows // cols
    bands = []
    for p in range(ny):
        block = flipped(gy, p)
        x_of, at = block // per, pl.multiple_of((block % per) * cols, cols)
        bands.append(
            jnp.concatenate([parts[x_of, m, pl.ds(at, cols), :] for m in range(ny)], axis=1)
        )
    a = jnp.concatenate(bands, axis=0) * (1.0 / 2.0**SQUARINGS)
    unit = jnp.where(
        lax.broadcasted_iota(jnp.int32, (order, order), 0)
        == lax.broadcasted_iota(jnp.int32, (order, order), 1),
        1.0, 0.0,
    )
    a_s = split(a)
    a2 = times(a_s, a_s)
    a4 = times(split(a2), split(X1 * a + X2 * a2))
    left = X3 * a2 + a4
    right = X5 * a + X6 * a2 + X7 * a4
    t = times(split(left), split(right)) + (unit + a + Y2 * a2 + X4 * left)
    for _ in range(SQUARINGS - 2):
        t_s = split(t)
        t = times(t_s, t_s)
    th[...], tl[...] = split(t)
    row_h, row_l = [], []
    for r in range(per):
        block = gx * per + r
        at, bit = 0, 1
        while bit < ny:
            at = at + ((block // bit + gy // bit) % 2) * bit
            bit *= 2
        at = pl.ds(pl.multiple_of(at * cols, cols), cols)
        row_h.append(th[at, :])
        row_l.append(tl[at, :])
    band = (jnp.concatenate(row_h, axis=0), jnp.concatenate(row_l, axis=0))
    full = (th[...], tl[...])
    column = (th[:, :cols], tl[:, :cols])
    out[...] = times(split(times(band, full)), split(times(full, column)))

    for copy in out_copies:
        copy.wait_send()
    for copy in passed:
        copy.wait_send()


def whole_on_each(nx, ny, generator):
    rows, cols = generator.shape
    order = ny * cols
    dma = pltpu.SemaphoreType.DMA
    return pl.pallas_call(
        functools.partial(whole_kernel, nx, ny),
        out_shape=jax.ShapeDtypeStruct((rows, cols), jnp.float32),
        in_specs=[pl.BlockSpec(memory_space=pl.ANY)],
        out_specs=pl.BlockSpec(memory_space=pltpu.VMEM),
        scratch_shapes=[
            pltpu.VMEM((nx, ny, rows, cols), jnp.float32),
            pltpu.VMEM((order, order), jnp.bfloat16),
            pltpu.VMEM((order, order), jnp.bfloat16),
            dma((ny, CHUNKS)),
            dma((ny, CHUNKS)),
            dma((nx - 1, ny, CHUNKS)),
            dma((nx - 1, ny, CHUNKS)),
            dma,
        ],
        compiler_params=pltpu.CompilerParams(collective_id=0, has_side_effects=True),
    )(generator)


def multiply(first, second):
    return jnp.dot(
        first, second, precision=lax.Precision.HIGHEST, preferred_element_type=jnp.float32
    )


def product(first, second):
    column = lax.all_gather(second, "gx", axis=0, tiled=True)
    return multiply(lax.all_gather(first, "gy", axis=1, tiled=True), column)


def in_blocks(generator):
    rows, cols = generator.shape
    row_ids = lax.broadcasted_iota(jnp.int32, (rows, cols), 0) + lax.axis_index("gx") * rows
    col_ids = lax.broadcasted_iota(jnp.int32, (rows, cols), 1) + lax.axis_index("gy") * cols
    unit = jnp.where(row_ids == col_ids, 1.0, 0.0).astype(jnp.float32)
    a = generator / 2.0**SQUARINGS
    a2 = product(a, a)
    a4 = product(a2, X1 * a + X2 * a2)
    left = X3 * a2 + a4
    t = product(left, X5 * a + X6 * a2 + X7 * a4) + (unit + a + Y2 * a2 + X4 * left)
    for _ in range(SQUARINGS):
        t = product(t, t)
    return t


def solution(mesh):
    nx, ny = mesh.shape["gx"], mesh.shape["gy"]

    def shards(generator):
        rows, cols = generator.shape
        fits = 12 * 4 * (nx * rows) * (ny * cols) <= VMEM_BUDGET
        square = nx * rows == ny * cols and rows % cols == 0
        if fits and square and ny & (ny - 1) == 0 and rows % (8 * CHUNKS) == 0 and cols % 16 == 0:
            return whole_on_each(nx, ny, generator)
        return in_blocks(generator)

    return jax.shard_map(
        shards, mesh=mesh, in_specs=(P("gx", "gy"),), out_specs=P("gx", "gy"), check_vma=False
    )
```

```python
import functools
import math

import jax
import jax.numpy as jnp
from jax import lax
from jax.experimental import pallas as pl
from jax.experimental.pallas import tpu as pltpu
from jax.sharding import PartitionSpec as P

DEGREE = 8
SQUARINGS = 4
CHUNKS = 2
LANES = 128
MATMUL = 256
VMEM_BUDGET = 40 * 2**20

ROOT = math.sqrt(177.0)
X3 = 2.0 / 3.0
X1 = X3 * (1.0 + ROOT) / 88.0
X2 = X3 * (1.0 + ROOT) / 352.0
X4 = (-271.0 + 29.0 * ROOT) / (315.0 * X3)
X5 = 11.0 * (-1.0 + ROOT) / (1260.0 * X3)
X6 = 11.0 * (-9.0 + ROOT) / (5040.0 * X3)
X7 = (89.0 - ROOT) / (5040.0 * X3 * X3)
Y2 = (857.0 - 58.0 * ROOT) / 630.0


def split(x):
    high = x.astype(jnp.bfloat16)
    return high, (x - high.astype(jnp.float32)).astype(jnp.bfloat16)


def times(x, y):
    dot = functools.partial(jnp.dot, preferred_element_type=jnp.float32)
    both = jnp.concatenate(x, axis=1)
    width = y[0].shape[1]
    whole = width // MATMUL * MATMUL
    if width - whole > MATMUL // 2:
        whole = width
    done = []
    if whole:
        high, low = y[0][:, :whole], y[1][:, :whole]
        done.append(dot(both, jnp.concatenate([high, high], axis=0)) + dot(x[0], low))
    if whole < width:
        high, low = y[0][:, whole:], y[1][:, whole:]
        pair = jnp.concatenate(
            [
                jnp.concatenate([high, low], axis=1),
                jnp.concatenate([high, jnp.zeros_like(low)], axis=1),
            ],
            axis=0,
        )
        two = dot(both, pair)
        done.append(two[:, : width - whole] + two[:, width - whole :])
    return done[0] if len(done) == 1 else jnp.concatenate(done, axis=1)


def flipped(index, mask):
    bit = 1
    while bit <= mask:
        if mask & bit:
            index = index + (1 - 2 * ((index // bit) % 2)) * bit
        bit *= 2
    return index


def packed(x):
    cols = x.shape[1]
    free = LANES - cols
    tail = x.shape[0] * free // LANES
    body = x.shape[0] - tail
    side = jnp.concatenate([x[body:, k : k + free] for k in range(0, cols, free)], axis=0)
    return jnp.concatenate([x[:body], side], axis=1)


def unpacked(x, cols):
    tail = x.shape[0] * (LANES - cols) // cols
    side = [x[k : k + tail, cols:] for k in range(0, x.shape[0], tail)]
    return jnp.concatenate([x[:, :cols], jnp.concatenate(side, axis=1)], axis=0)


def whole_kernel(nx, ny, gen, out, local, parts, af, th, tl, send, land, relay, relayed, own):
    rows, cols = out.shape
    order = ny * cols
    per = rows // cols
    span = parts.shape[2] // CHUNKS
    gx, gy = lax.axis_index("gx"), lax.axis_index("gy")

    barrier = pltpu.get_barrier_semaphore()
    mine = pltpu.make_async_copy(gen, local, own)
    mine.start()
    for mask in range(1, ny):
        pl.semaphore_signal(barrier, inc=1, device_id={"gy": flipped(gy, mask)})
    for dx in range(1, nx):
        pl.semaphore_signal(barrier, inc=1, device_id={"gx": (gx + dx) % nx})
    mine.wait()
    parts[gx, 0] = packed(local[...])
    pl.semaphore_wait(barrier, ny + nx - 2)

    out_copies, passed = [], []

    def pass_on(mask, c):
        piece = parts.at[gx, mask, pl.ds(c * span, span), :]
        for dx in range(1, nx):
            copy = pltpu.make_async_remote_copy(
                piece, piece, relay.at[dx - 1, mask, c], relayed.at[dx - 1, mask, c],
                device_id={"gx": (gx + dx) % nx},
            )
            copy.start()
            passed.append(copy)

    for c in range(CHUNKS):
        piece = pl.ds(c * span, span)
        for mask in range(ny - 1, 0, -1):
            copy = pltpu.make_async_remote_copy(
                parts.at[gx, 0, piece, :], parts.at[gx, mask, piece, :],
                send.at[mask, c], land.at[mask, c],
                device_id={"gy": flipped(gy, mask)},
            )
            copy.start()
            out_copies.append(copy)
    for c in range(CHUNKS):
        pass_on(0, c)
    for c in range(CHUNKS):
        for mask in range(1, ny):
            out_copies[c * (ny - 1) + ny - 1 - mask].wait_recv()
            pass_on(mask, c)
    for copy in passed:
        copy.wait_recv()

    def place(block):
        at, bit = 0, 1
        while bit < ny:
            at = at + ((block // bit + gy // bit) % 2) * bit
            bit *= 2
        return pl.ds(pl.multiple_of(at * cols, cols), cols)

    for x in range(nx):
        band = jnp.concatenate([unpacked(parts[x, m], cols) for m in range(ny)], axis=1)
        band = band * (1.0 / 2.0**SQUARINGS)
        for r in range(per):
            af[place(x * per + r), :] = band[r * cols : (r + 1) * cols]
    a = af[...]
    unit = jnp.where(
        lax.broadcasted_iota(jnp.int32, (order, order), 0)
        == lax.broadcasted_iota(jnp.int32, (order, order), 1),
        1.0, 0.0,
    )
    a_s = split(a)
    a2 = times(a_s, a_s)
    a4 = times(split(a2), split(X1 * a + X2 * a2))
    left = X3 * a2 + a4
    right = X5 * a + X6 * a2 + X7 * a4
    t = times(split(left), split(right)) + (unit + a + Y2 * a2 + X4 * left)
    for _ in range(SQUARINGS - 2):
        t_s = split(t)
        t = times(t_s, t_s)
    th[...], tl[...] = split(t)
    rows_at = [place(gx * per + r) for r in range(per)]
    band = tuple(jnp.concatenate([t[at, :] for at in rows_at], axis=0) for t in (th, tl))
    full = (th[...], tl[...])
    column = (th[:, :LANES], tl[:, :LANES])
    out[...] = times(split(times(band, full)), split(times(full, column)))[:, :cols]

    for copy in out_copies:
        copy.wait_send()
    for copy in passed:
        copy.wait_send()


def whole_on_each(nx, ny, generator):
    rows, cols = generator.shape
    order = ny * cols
    dma = pltpu.SemaphoreType.DMA
    return pl.pallas_call(
        functools.partial(whole_kernel, nx, ny),
        out_shape=jax.ShapeDtypeStruct((rows, cols), jnp.float32),
        in_specs=[pl.BlockSpec(memory_space=pl.ANY)],
        out_specs=pl.BlockSpec(memory_space=pltpu.VMEM),
        scratch_shapes=[
            pltpu.VMEM((rows, cols), jnp.float32),
            pltpu.VMEM((nx, ny, rows * cols // LANES, LANES), jnp.float32),
            pltpu.VMEM((order, order), jnp.float32),
            pltpu.VMEM((order, order), jnp.bfloat16),
            pltpu.VMEM((order, order), jnp.bfloat16),
            dma((ny, CHUNKS)),
            dma((ny, CHUNKS)),
            dma((nx - 1, ny, CHUNKS)),
            dma((nx - 1, ny, CHUNKS)),
            dma,
        ],
        compiler_params=pltpu.CompilerParams(collective_id=0, has_side_effects=True),
    )(generator)


def multiply(first, second):
    return jnp.dot(
        first, second, precision=lax.Precision.HIGHEST, preferred_element_type=jnp.float32
    )


def product(first, second):
    column = lax.all_gather(second, "gx", axis=0, tiled=True)
    return multiply(lax.all_gather(first, "gy", axis=1, tiled=True), column)


def in_blocks(generator):
    rows, cols = generator.shape
    row_ids = lax.broadcasted_iota(jnp.int32, (rows, cols), 0) + lax.axis_index("gx") * rows
    col_ids = lax.broadcasted_iota(jnp.int32, (rows, cols), 1) + lax.axis_index("gy") * cols
    unit = jnp.where(row_ids == col_ids, 1.0, 0.0).astype(jnp.float32)
    a = generator / 2.0**SQUARINGS
    a2 = product(a, a)
    a4 = product(a2, X1 * a + X2 * a2)
    left = X3 * a2 + a4
    t = product(left, X5 * a + X6 * a2 + X7 * a4) + (unit + a + Y2 * a2 + X4 * left)
    for _ in range(SQUARINGS):
        t = product(t, t)
    return t


def solution(mesh):
    nx, ny = mesh.shape["gx"], mesh.shape["gy"]

    def shards(generator):
        rows, cols = generator.shape
        fits = 12 * 4 * (nx * rows) * (ny * cols) <= VMEM_BUDGET
        square = nx * rows == ny * cols and rows % cols == 0
        order_of = ny * cols
        free = LANES - cols
        packs = free > 0 and cols % free == 0 and rows * free % (LANES * 8 * CHUNKS) == 0
        if fits and square and ny & (ny - 1) == 0 and packs and cols % 16 == 0 and order_of % LANES == 0:
            return whole_on_each(nx, ny, generator)
        return in_blocks(generator)

    return jax.shard_map(
        shards, mesh=mesh, in_specs=(P("gx", "gy"),), out_specs=P("gx", "gy"), check_vma=False
    )
```

```python
import functools
import math

import jax
import jax.numpy as jnp
from jax import lax
from jax.experimental import pallas as pl
from jax.experimental.pallas import tpu as pltpu
from jax.sharding import PartitionSpec as P

DEGREE = 8
SQUARINGS = 4
CHUNKS = 2
LANES = 128
MATMUL = 256
VMEM_BUDGET = 40 * 2**20

ROOT = math.sqrt(177.0)
X3 = 2.0 / 3.0
X1 = X3 * (1.0 + ROOT) / 88.0
X2 = X3 * (1.0 + ROOT) / 352.0
X4 = (-271.0 + 29.0 * ROOT) / (315.0 * X3)
X5 = 11.0 * (-1.0 + ROOT) / (1260.0 * X3)
X6 = 11.0 * (-9.0 + ROOT) / (5040.0 * X3)
X7 = (89.0 - ROOT) / (5040.0 * X3 * X3)
Y2 = (857.0 - 58.0 * ROOT) / 630.0


def split(x):
    high = x.astype(jnp.bfloat16)
    return high, (x - high.astype(jnp.float32)).astype(jnp.bfloat16)


def times(x, y):
    dot = functools.partial(jnp.dot, preferred_element_type=jnp.float32)
    both = jnp.concatenate(x, axis=1)
    width = y[0].shape[1]
    whole = width // MATMUL * MATMUL
    if width - whole > MATMUL // 2:
        whole = width
    done = []
    if whole:
        high, low = y[0][:, :whole], y[1][:, :whole]
        done.append(dot(both, jnp.concatenate([high, high], axis=0)) + dot(x[0], low))
    if whole < width:
        high, low = y[0][:, whole:], y[1][:, whole:]
        pair = jnp.concatenate(
            [
                jnp.concatenate([high, low], axis=1),
                jnp.concatenate([high, jnp.zeros_like(low)], axis=1),
            ],
            axis=0,
        )
        two = dot(both, pair)
        done.append(two[:, : width - whole] + two[:, width - whole :])
    return done[0] if len(done) == 1 else jnp.concatenate(done, axis=1)


def flipped(index, mask):
    bit = 1
    while bit <= mask:
        if mask & bit:
            index = index + (1 - 2 * ((index // bit) % 2)) * bit
        bit *= 2
    return index


def packed(x):
    cols = x.shape[1]
    free = LANES - cols
    tail = x.shape[0] * free // LANES
    body = x.shape[0] - tail
    side = jnp.concatenate([x[body:, k : k + free] for k in range(0, cols, free)], axis=0)
    return jnp.concatenate([x[:body], side], axis=1)


def unpacked(x, cols):
    tail = x.shape[0] * (LANES - cols) // cols
    side = [x[k : k + tail, cols:] for k in range(0, x.shape[0], tail)]
    return jnp.concatenate([x[:, :cols], jnp.concatenate(side, axis=1)], axis=0)


def whole_kernel(nx, ny, gen, out, local, parts, af, th, tl, send, land, relay, relayed, own):
    rows, cols = out.shape
    order = ny * cols
    per = rows // cols
    span = parts.shape[2] // CHUNKS
    gx, gy = lax.axis_index("gx"), lax.axis_index("gy")

    barrier = pltpu.get_barrier_semaphore()
    mine = pltpu.make_async_copy(gen, local, own)
    mine.start()
    for mask in range(1, ny):
        pl.semaphore_signal(barrier, inc=1, device_id={"gy": flipped(gy, mask)})
    for dx in range(1, nx):
        pl.semaphore_signal(barrier, inc=1, device_id={"gx": (gx + dx) % nx})
    mine.wait()
    parts[gx, 0] = packed(local[...])
    pl.semaphore_wait(barrier, ny + nx - 2)

    out_copies, passed = [], []

    def pass_on(mask, c):
        piece = parts.at[gx, mask, pl.ds(c * span, span), :]
        for dx in range(1, nx):
            copy = pltpu.make_async_remote_copy(
                piece, piece, relay.at[dx - 1, mask, c], relayed.at[dx - 1, mask, c],
                device_id={"gx": (gx + dx) % nx},
            )
            copy.start()
            passed.append(copy)

    for c in range(CHUNKS):
        piece = pl.ds(c * span, span)
        for mask in range(ny - 1, 0, -1):
            copy = pltpu.make_async_remote_copy(
                parts.at[gx, 0, piece, :], parts.at[gx, mask, piece, :],
                send.at[mask, c], land.at[mask, c],
                device_id={"gy": flipped(gy, mask)},
            )
            copy.start()
            out_copies.append(copy)
    for c in range(CHUNKS):
        pass_on(0, c)
    for c in range(CHUNKS):
        for mask in range(1, ny):
            out_copies[c * (ny - 1) + ny - 1 - mask].wait_recv()
            pass_on(mask, c)
    for copy in passed:
        copy.wait_recv()

    def place(block):
        at, bit = 0, 1
        while bit < ny:
            at = at + ((block // bit + gy // bit) % 2) * bit
            bit *= 2
        return pl.ds(pl.multiple_of(at * cols, cols), cols)

    for x in range(nx):
        band = jnp.concatenate([unpacked(parts[x, m], cols) for m in range(ny)], axis=1)
        band = band * (1.0 / 2.0**SQUARINGS)
        for r in range(per):
            af[place(x * per + r), :] = band[r * cols : (r + 1) * cols]
    a = af[...]
    unit = jnp.where(
        lax.broadcasted_iota(jnp.int32, (order, order), 0)
        == lax.broadcasted_iota(jnp.int32, (order, order), 1),
        1.0, 0.0,
    )
    a_s = split(a)
    a2 = times(a_s, a_s)
    a4 = times(split(a2), split(X1 * a + X2 * a2))
    left = X3 * a2 + a4
    right = X5 * a + X6 * a2 + X7 * a4
    t = times(split(left), split(right)) + (unit + a + Y2 * a2 + X4 * left)
    for _ in range(SQUARINGS - 2):
        t_s = split(t)
        t = times(t_s, t_s)
    th[...], tl[...] = split(t)
    rows_at = [place(gx * per + r) for r in range(per)]
    band = tuple(jnp.concatenate([t[at, :] for at in rows_at], axis=0) for t in (th, tl))
    full = (th[...], tl[...])
    column = (th[:, :LANES], tl[:, :LANES])
    out[...] = times(split(times(band, full)), split(times(full, column)))[:, :cols]

    for copy in out_copies:
        copy.wait_send()
    for copy in passed:
        copy.wait_send()


def whole_on_each(nx, ny, generator):
    rows, cols = generator.shape
    order = ny * cols
    dma = pltpu.SemaphoreType.DMA
    return pl.pallas_call(
        functools.partial(whole_kernel, nx, ny),
        out_shape=pltpu.VMEM((rows, cols), jnp.float32),
        in_specs=[pl.BlockSpec(memory_space=pl.ANY)],
        out_specs=pl.BlockSpec(memory_space=pltpu.VMEM),
        scratch_shapes=[
            pltpu.VMEM((rows, cols), jnp.float32),
            pltpu.VMEM((nx, ny, rows * cols // LANES, LANES), jnp.float32),
            pltpu.VMEM((order, order), jnp.float32),
            pltpu.VMEM((order, order), jnp.bfloat16),
            pltpu.VMEM((order, order), jnp.bfloat16),
            dma((ny, CHUNKS)),
            dma((ny, CHUNKS)),
            dma((nx - 1, ny, CHUNKS)),
            dma((nx - 1, ny, CHUNKS)),
            dma,
        ],
        compiler_params=pltpu.CompilerParams(collective_id=0, has_side_effects=True),
    )(generator)


def multiply(first, second):
    return jnp.dot(
        first, second, precision=lax.Precision.HIGHEST, preferred_element_type=jnp.float32
    )


def product(first, second):
    column = lax.all_gather(second, "gx", axis=0, tiled=True)
    return multiply(lax.all_gather(first, "gy", axis=1, tiled=True), column)


def in_blocks(generator):
    rows, cols = generator.shape
    row_ids = lax.broadcasted_iota(jnp.int32, (rows, cols), 0) + lax.axis_index("gx") * rows
    col_ids = lax.broadcasted_iota(jnp.int32, (rows, cols), 1) + lax.axis_index("gy") * cols
    unit = jnp.where(row_ids == col_ids, 1.0, 0.0).astype(jnp.float32)
    a = generator / 2.0**SQUARINGS
    a2 = product(a, a)
    a4 = product(a2, X1 * a + X2 * a2)
    left = X3 * a2 + a4
    t = product(left, X5 * a + X6 * a2 + X7 * a4) + (unit + a + Y2 * a2 + X4 * left)
    for _ in range(SQUARINGS):
        t = product(t, t)
    return t


def solution(mesh):
    nx, ny = mesh.shape["gx"], mesh.shape["gy"]

    def shards(generator):
        rows, cols = generator.shape
        fits = 12 * 4 * (nx * rows) * (ny * cols) <= VMEM_BUDGET
        square = nx * rows == ny * cols and rows % cols == 0
        order_of = ny * cols
        free = LANES - cols
        packs = free > 0 and cols % free == 0 and rows * free % (LANES * 8 * CHUNKS) == 0
        if fits and square and ny & (ny - 1) == 0 and packs and cols % 16 == 0 and order_of % LANES == 0:
            return whole_on_each(nx, ny, generator)
        return in_blocks(generator)

    return jax.shard_map(
        shards, mesh=mesh, in_specs=(P("gx", "gy"),), out_specs=P("gx", "gy"), check_vma=False
    )
```
